8 devices in a mesh: rep: 2 (over y, z), dp: 4 (over x, core).
Axes of the slice: x: 2, y: 2, z: 1, core: 2. Of those that a mesh axis runs over, the one named last changes fastest.
Arguments:
- x: bfloat16 [8, 2048, 768], P(('rep', 'dp')), parts along dimension 0
- dy: bfloat16 [8, 2048, 768], P(('rep', 'dp')), parts along dimension 0
- w_gate: bfloat16 [2, 768, 3072], replicated
- w_up: bfloat16 [2, 768, 3072], replicated
- w_down: bfloat16 [2, 3072, 768], replicated
- m_w_gate: float32 [2, 768, 3072], P(None, 'dp')
- m_w_up: float32 [2, 768, 3072], P(None, 'dp')
- m_w_down: float32 [2, 3072, 768], P(None, 'dp')
- v_w_gate: float32 [2, 768, 3072], P(None, 'dp')
- v_w_up: float32 [2, 768, 3072], P(None, 'dp')
- v_w_down: float32 [2, 3072, 768], P(None, 'dp')
Outputs:
- output 1: bfloat16 [4, 768, 3072], P('rep'), parts along dimension 0
- output 2: bfloat16 [4, 768, 3072], P('rep'), parts along dimension 0
- output 3: bfloat16 [4, 3072, 768], P('rep'), parts along dimension 0
- output 4: float32 [4, 768, 3072], P('rep', 'dp'), parts along dimension 0
- output 5: float32 [4, 768, 3072], P('rep', 'dp'), parts along dimension 0
- output 6: float32 [4, 3072, 768], P('rep', 'dp'), parts along dimension 0
- output 7: float32 [4, 768, 3072], P('rep', 'dp'), parts along dimension 0
- output 8: float32 [4, 768, 3072], P('rep', 'dp'), parts along dimension 0
- output 9: float32 [4, 3072, 768], P('rep', 'dp'), parts along dimension 0
There are 2 independent parts. The reference program is written for one: setup_inputs(seed, part) draws one part's arguments, and reference() takes and returns one part's arrays. A program takes and returns all parts, laid end to end along the dimension named above; an argument that names none is the same for every part.
All inputs are finite; a program needn't handle non-finite values.
Results may differ from the reference program's by a relative error of at most 0.022.
Values are sent between devices in bfloat16 or wider.
A program may use at most 2 GiB of HBM per device.

```python
import jax
import jax.numpy as jnp
from jax import lax

SEQUENCES = 4
TOKENS = 2048
D = 768
FF = 3072
LAYERS = 2
NAMES = ("w_gate", "w_up", "w_down")
SHAPES = {"w_gate": (LAYERS, D, FF), "w_up": (LAYERS, D, FF), "w_down": (LAYERS, FF, D)}


def bump(key, n, height):
    away = (jnp.arange(n, dtype=jnp.int32) - jax.random.randint(key, (), 0, n, jnp.int32)) % n
    return jnp.where(away < n // 8, height, 1.0)


def together(key, own, strength):
    shared = jax.random.normal(key, own.shape[1:], jnp.float32)
    return (own + strength * shared) * lax.rsqrt(1 + strength * strength)


def setup_inputs(seed: int = 0, part: int = 0) -> dict:
    kx, kdy, ka, kb, kz, kf, kh, kl, *keys = jax.random.split(jax.random.key(seed), 8 + 3 * len(NAMES))
    kx, kdy, ka, kb = (jax.random.fold_in(k, part) for k in (kx, kdy, ka, kb))
    kw, km, kv = (keys[i::3] for i in range(3))
    shape = (SEQUENCES, TOKENS, D)
    much_x, much_dy = jax.random.uniform(kz, (2,), jnp.float32, 0.0, 1.0)
    loud = 2.0 ** jax.random.uniform(jax.random.fold_in(kz, 1), (), jnp.float32, -1.0, 2.0)
    layers = 2.0 ** jax.random.uniform(kl, (LAYERS, 1, 1), jnp.float32, -1.0, 1.0)
    x = together(ka, jax.random.normal(kx, shape, jnp.float32), much_x) * bump(kf, D, 4.0)
    dy = together(kb, jax.random.normal(kdy, shape, jnp.float32), much_dy)
    drawn = {"x": x.astype(jnp.bfloat16), "dy": (loud * dy * (SEQUENCES * TOKENS) ** -0.5).astype(jnp.bfloat16)}
    for key, name in zip(kw, NAMES, strict=True):
        w = jax.random.normal(key, SHAPES[name], jnp.float32) * SHAPES[name][1] ** -0.5
        drawn[name] = (w * {"w_gate": 1.0, "w_up": bump(kh, FF, 4.0), "w_down": layers}[name]).astype(jnp.bfloat16)
    for key, name in zip(km, NAMES, strict=True):
        drawn[f"m_{name}"] = 0.1 * jax.random.normal(key, SHAPES[name], jnp.float32)
    for key, name in zip(kv, NAMES, strict=True):
        drawn[f"v_{name}"] = jax.random.uniform(key, SHAPES[name], jnp.float32, 0.005, 0.015)
    return drawn


def matmul(a, w):
    return jnp.dot(a, w, preferred_element_type=jnp.float32).astype(jnp.bfloat16)


def normed(h):
    wide = h.astype(jnp.float32)
    scale = lax.rsqrt(jnp.mean(wide**2, -1, keepdims=True) + 1e-6)
    return (wide * scale).astype(jnp.bfloat16)


def layer(h, w):
    a = normed(h)
    gate = jnp.dot(a, w["w_gate"], preferred_element_type=jnp.float32)
    up = jnp.dot(a, w["w_up"], preferred_element_type=jnp.float32)
    return h + matmul((jax.nn.silu(gate) * up).astype(jnp.bfloat16), w["w_down"])


def adamw(w, m, v, g):
    m = 0.9 * m + 0.1 * g
    v = 0.95 * v + 0.05 * g * g
    step = m * lax.rsqrt(v + 1e-8) + 0.1 * w
    return (w - 0.02 * step).astype(jnp.bfloat16), m, v


def stack(weights, h):
    return lax.scan(lambda h, w: (layer(h, w), None), h, weights)[0]


def reference(x, dy, w_gate, w_up, w_down, m_w_gate, m_w_up, m_w_down, v_w_gate, v_w_up, v_w_down):
    weights = dict(zip(NAMES, (w_gate, w_up, w_down), strict=True))

    def take(so_far, sequence):
        h, by_y = sequence
        _, back = jax.vjp(lambda w: stack(w, h), weights)
        return jax.tree.map(lambda total, term: total + term.astype(jnp.float32), so_far, back(by_y)[0]), None

    none_yet = {name: jnp.zeros(w.shape, jnp.float32) for name, w in weights.items()}
    by_weights, _ = lax.scan(take, none_yet, (x, dy))
    gradients = [by_weights[name].astype(jnp.bfloat16).astype(jnp.float32) for name in NAMES]
    new = [
        adamw(w.astype(jnp.float32), m, v, g)
        for w, m, v, g in zip((w_gate, w_up, w_down), (m_w_gate, m_w_up, m_w_down), (v_w_gate, v_w_up, v_w_down), gradients, strict=True)
    ]
    return tuple(one[which] for which in range(3) for one in new)
```

```python
import jax
import jax.numpy as jnp
from jax import lax
from jax.sharding import PartitionSpec as P

NAMES = ("w_gate", "w_up", "w_down")
SIBLING = [(i, i ^ 1) for i in range(4)]
CROSS = [(i, i ^ 2) for i in range(4)]
BF, F32 = jnp.bfloat16, jnp.float32


def dot(a, b, dims, out=BF):
    return lax.dot_general(a, b, (dims, ((), ())), preferred_element_type=F32).astype(out)


def normed(h):
    wide = h.astype(F32)
    scale = lax.rsqrt(jnp.mean(wide**2, -1, keepdims=True) + 1e-6)
    return (wide * scale).astype(BF)


def adamw(w, m, v, g):
    m = 0.9 * m + 0.1 * g
    v = 0.95 * v + 0.05 * g * g
    step = m * lax.rsqrt(v + 1e-8) + 0.1 * w
    return (w - 0.02 * step).astype(BF), m, v


def gated(gate, up):
    return (jax.nn.silu(gate) * up).astype(BF)


def solution(mesh):
    def body(x, dy, wg, wu, wd, mg, mu, md, vg, vu, vd):
        x, dy = x[0], dy[0]
        dp = lax.axis_index("dp")
        side, core = dp // 2, dp % 2
        ws, ms, vs = (wg, wu, wd), (mg, mu, md), (vg, vu, vd)

        def reduce(g):
            rows, cols = g.shape
            g = g.reshape(2, 2, rows // 4, cols)
            mine = lax.dynamic_index_in_dim(g, core, 1, keepdims=False)
            out = lax.dynamic_index_in_dim(g, 1 - core, 1, keepdims=False)
            got = lax.ppermute(out, "dp", SIBLING)
            both = mine.astype(F32) + got.astype(F32)
            own = lax.dynamic_index_in_dim(both, side, 0, keepdims=False)
            send = lax.dynamic_index_in_dim(both, 1 - side, 0, keepdims=False).astype(BF)
            return own + lax.ppermute(send, "dp", CROSS).astype(F32)

        new = {}

        def update(layer, i, g):
            g = reduce(g).astype(BF).astype(F32)
            rows = g.shape[0]
            w = lax.dynamic_slice_in_dim(ws[i][layer], dp * rows, rows, 0).astype(F32)
            nw, nm, nv = adamw(w, ms[i][layer], vs[i][layer], g)
            far = lax.ppermute(nw, "dp", CROSS)
            near = lax.ppermute(nw, "dp", SIBLING)
            diagonal = lax.ppermute(far, "dp", SIBLING)
            new[layer, i] = (nw, near, far, diagonal), nm, nv

        h = [x]
        saved = []
        for n in range(2):
            a = normed(h[n])
            gate = dot(a, wg[n], ((1,), (0,)), F32)
            up = dot(a, wu[n], ((1,), (0,)), F32)
            act = gated(gate, up)
            saved.append((a, gate, up, act))
            if n == 0:
                h.append(h[0] + dot(act, wd[0], ((1,), (0,))))
        d = dy
        for n in (1, 0):
            a, gate, up, act = saved[n]
            update(n, 2, dot(act, d, ((0,), (0,))))
            dact = dot(d, wd[n], ((1,), (1,)))
            dgate, dup = jax.vjp(gated, gate, up)[1](dact)
            dgate, dup = dgate.astype(BF), dup.astype(BF)
            update(n, 0, dot(a, dgate, ((0,), (0,))))
            update(n, 1, dot(a, dup, ((0,), (0,))))
            if n:
                da = dot(dgate, wg[n], ((1,), (1,))) + dot(dup, wu[n], ((1,), (1,)))
                d = d + jax.vjp(normed, h[n])[1](da)[0]

        outs_w = []
        for i in range(3):
            layers = []
            for n in range(2):
                nw, near, far, diagonal = new[n, i][0]
                stacked = jnp.zeros((4, *nw.shape), BF)
                for piece, who in ((nw, dp), (near, dp ^ 1), (far, dp ^ 2), (diagonal, dp ^ 3)):
                    stacked = lax.dynamic_update_index_in_dim(stacked, piece, who, 0)
                layers.append(stacked.reshape(-1, nw.shape[1]))
            outs_w.append(jnp.stack(layers))
        outs_m = [jnp.stack([new[n, i][1] for n in range(2)]) for i in range(3)]
        outs_v = [jnp.stack([new[n, i][2] for n in range(2)]) for i in range(3)]
        return (*outs_w, *outs_m, *outs_v)

    batch, whole, rows = P(("rep", "dp")), P(), P(None, "dp")
    return jax.shard_map(
        body,
        mesh=mesh,
        in_specs=(batch, batch, *(whole,) * 3, *(rows,) * 6),
        out_specs=(*(P("rep"),) * 3, *(P("rep", "dp"),) * 6),
        check_vma=False,
    )
```

```python
import functools

import jax
import jax.numpy as jnp
from jax import lax
from jax.experimental import pallas as pl
from jax.experimental.pallas import tpu as pltpu
from jax.sharding import PartitionSpec as P


SIBLING = [(i, i ^ 1) for i in range(4)]
CROSS = [(i, i ^ 2) for i in range(4)]
BF, F32 = jnp.bfloat16, jnp.float32
T, D, FF, N = 2048, 768, 3072, 4
TILE = FF // N

def mm(a, b, ca=1, cb=0):
    return lax.dot_general(a, b, (((ca,), (cb,)), ((), ())), preferred_element_type=F32)

def norm(h):
    wide = h.astype(F32)
    return (wide * lax.rsqrt(jnp.mean(wide * wide, -1, keepdims=True) + 1e-6)).astype(BF)

def params(mib=63, n=1):
    return pltpu.CompilerParams(dimension_semantics=("arbitrary",) * n, vmem_limit_bytes=mib * 2**20)

def cost(mms):
    return pl.CostEstimate(flops=int(mms * 2 * T * D * FF), bytes_accessed=int(2e7), transcendentals=0)

def once(shape, index):
    return pl.BlockSpec(shape, index, pipeline_mode=pl.Buffered(1))

def fwd_body(x_ref, wg_ref, wu_ref, wd_ref, g_ref, u_ref, a_ref, h_ref, b_ref):
    x = x_ref[...]
    a = norm(x)
    a_ref[...] = a
    acc = None
    for f in range(N):
        at = slice(f * TILE, (f + 1) * TILE)
        g = mm(a, wg_ref[0, :, at])
        u = mm(a, wu_ref[0, :, at])
        g_ref[:, at] = g
        u_ref[:, at] = u
        act = (g * jax.nn.sigmoid(g) * u).astype(BF)
        p = mm(act, wd_ref[0, at, :])
        acc = p if acc is None else acc + p
    h = x + acc.astype(BF)
    h_ref[...] = h
    b_ref[...] = norm(h)

def fwd(x, wg, wu, wd, mb=512):
    row = lambda c: pl.BlockSpec((mb, c), lambda m: (m, 0))
    sds = jax.ShapeDtypeStruct
    return pl.pallas_call(fwd_body, grid=(T // mb,),
        in_specs=[row(D), once((1, D, FF), lambda m: (0, 0, 0)), once((1, D, FF), lambda m: (0, 0, 0)), once((1, FF, D), lambda m: (0, 0, 0))],
        out_specs=[row(FF), row(FF), row(D), row(D), row(D)],
        out_shape=[sds((T, FF), F32), sds((T, FF), F32), sds((T, D), BF), sds((T, D), BF), sds((T, D), BF)],
        compiler_params=params(), cost_estimate=cost(3), name="fwd")(x, wg, wu, wd)

def gate_bwd(g, u, dact):
    s = jax.nn.sigmoid(g)
    silu = g * s
    d = dact.astype(BF).astype(F32)
    dup = (d * silu).astype(BF)
    dgate = (d * u * (s + silu * (1.0 - s))).astype(BF)
    return silu, dgate, dup

def back_body(recompute, q_ref, d_ref, a_ref, *refs):
    if recompute:
        wg_ref, wu_ref, wd_ref, act_ref, dg_ref, du_ref, keep_ref, send_ref, accg, accu = refs
    else:
        g_ref, u_ref, wd_ref, act_ref, keep_ref, send_ref, accg, accu = refs
    m = pl.program_id(0)
    a = a_ref[...]
    if recompute:
        g = mm(a, wg_ref[0])
        u = mm(a, wu_ref[0])
    else:
        g, u = g_ref[...], u_ref[...]
    dact = mm(d_ref[...], wd_ref[0], 1, 1)
    silu, dgate, dup = gate_bwd(g, u, dact)
    act_ref[...] = (silu * u).astype(BF)
    if recompute:
        dg_ref[...] = dgate
        du_ref[...] = dup
    pg = mm(a, dgate, 0, 0)
    pu = mm(a, dup, 0, 0)

    @pl.when(m == 0)
    def _():
        accg[...] = pg
        accu[...] = pu

    @pl.when(m > 0)
    def _():
        accg[...] += pg
        accu[...] += pu

    @pl.when(m == pl.num_programs(0) - 1)
    def _():
        core = q_ref[0] % 2
        rows = D // 4
        for side in range(2):
            mine = pl.ds(pl.multiple_of((2 * side + core) * rows, 64), rows)
            other = pl.ds(pl.multiple_of((2 * side + 1 - core) * rows, 64), rows)
            for i, acc in enumerate((accg, accu)):
                keep_ref[side, i] = acc[mine, :]
                send_ref[side, i] = acc[other, :].astype(BF)

def back(layer, t, q, d, a, first, second, wd, mb=512):
    sds = jax.ShapeDtypeStruct
    recompute = layer == 1
    row = lambda c: pl.BlockSpec((mb, c), lambda m, q: (m, 0))
    col = pl.BlockSpec((mb, TILE), lambda m, q: (m, t))
    wcol = once((1, D, TILE), lambda m, q: (layer, 0, t))
    wrow = once((1, TILE, D), lambda m, q: (layer, t, 0))
    extra = ([wcol, wcol] if recompute else [col, col]) + [wrow]
    whole = lambda *s: pl.BlockSpec(s, lambda m, q: (0,) * len(s))
    tile = sds((T, TILE), BF)
    outs = [tile] * (3 if recompute else 1)
    return pl.pallas_call(functools.partial(back_body, recompute),
        grid_spec=pltpu.PrefetchScalarGridSpec(num_scalar_prefetch=1, grid=(T // mb,),
            in_specs=[row(D), row(D), *extra],
            out_specs=[row(TILE)] * len(outs) + [whole(2, 2, D // 4, TILE)] * 2,
            scratch_shapes=[pltpu.VMEM((D, TILE), F32)] * 2),
        out_shape=[*outs, sds((2, 2, D // 4, TILE), F32), sds((2, 2, D // 4, TILE), BF)],
        compiler_params=params(), cost_estimate=cost(1.25 if recompute else 0.75))(q, d, a, first, second, wd)

def down_body(q_ref, a0, a1, a2, a3, d_ref, keep_ref, send_ref, acc):
    m = pl.program_id(0)
    d = d_ref[...]
    for t, a in enumerate((a0, a1, a2, a3)):
        p = mm(a[...], d, 0, 0)

        @pl.when(m == 0)
        def _():
            acc[t] = p

        @pl.when(m > 0)
        def _():
            acc[t] += p

    @pl.when(m == pl.num_programs(0) - 1)
    def _():
        core = q_ref[0] % 2
        for side in range(2):
            keep_ref[side] = acc[2 * side + core]
            send_ref[side] = acc[2 * side + 1 - core].astype(BF)

def down(q, acts, d, mb=512):
    sds = jax.ShapeDtypeStruct
    row = lambda c: pl.BlockSpec((mb, c), lambda m, q: (m, 0))
    whole = lambda *s: pl.BlockSpec(s, lambda m, q: (0,) * len(s))
    return pl.pallas_call(down_body,
        grid_spec=pltpu.PrefetchScalarGridSpec(num_scalar_prefetch=1, grid=(T // mb,),
            in_specs=[row(TILE)] * 4 + [row(D)], out_specs=[whole(2, TILE, D)] * 2,
            scratch_shapes=[pltpu.VMEM((4, TILE, D), F32)]),
        out_shape=[sds((2, TILE, D), F32), sds((2, TILE, D), BF)],
        compiler_params=params(), cost_estimate=cost(1), name="down")(q, *acts, d)

def input_body(dy_ref, h_ref, *refs):
    dgs, dus, (wg_ref, wu_ref, o_ref) = refs[:4], refs[4:8], refs[8:]
    da = None
    for ds, w in ((dgs, wg_ref), (dus, wu_ref)):
        s = None
        for t in range(4):
            p = mm(ds[t][...], w[0, :, t * TILE:(t + 1) * TILE], 1, 1)
            s = p if s is None else s + p
        s = s.astype(BF)
        da = s if da is None else da + s
    da = da.astype(F32)
    wide = h_ref[...].astype(F32)
    scale = lax.rsqrt(jnp.mean(wide * wide, -1, keepdims=True) + 1e-6)
    along = jnp.sum(da * wide, -1, keepdims=True)
    dh = da * scale - wide * (along * scale * scale * scale * (1.0 / D))
    o_ref[...] = dy_ref[...] + dh.astype(BF)

def input_grad(dy, h, dgs, dus, wg, wu, mb=512):
    row = lambda c: pl.BlockSpec((mb, c), lambda m: (m, 0))
    w = once((1, D, FF), lambda m: (1, 0, 0))
    return pl.pallas_call(input_body, grid=(T // mb,),
        in_specs=[row(D), row(D)] + [row(TILE)] * 8 + [w, w], out_specs=row(D),
        out_shape=jax.ShapeDtypeStruct((T, D), BF),
        compiler_params=params(), cost_estimate=cost(2), name="input_grad")(dy, h, *dgs, *dus, wg, wu)


def adamw(w, m, v, g):
    m = 0.9 * m + 0.1 * g
    v = 0.95 * v + 0.05 * g * g
    step = m * lax.rsqrt(v + 1e-8) + 0.1 * w
    return (w - 0.02 * step).astype(BF), m, v


def update_body(pairs, q_ref, keep_ref, near_ref, got_ref, *refs):
    ins, outs = refs[: 3 * pairs], refs[-(3 * pairs + 1) :]
    for i in range(pairs):
        w, m, v = ins[3 * i : 3 * i + 3]
        g = (keep_ref[0, i] + near_ref[0, i].astype(F32) + got_ref[i].astype(F32)).astype(BF).astype(F32)
        nw, nm, nv = adamw(w[0].astype(F32), m[0], v[0], g)
        outs[3 * i][0] = nw
        outs[3 * i + 1][0] = nm
        outs[3 * i + 2][0] = nv
        outs[-1][i] = nw


def update(layer, t, q, keep, near, got, arrays, chain):
    pairs = len(arrays) // 3
    sds = jax.ShapeDtypeStruct
    if pairs == 2:
        rows, width, steps = D // 4, TILE, 3
        part = width // steps
        mine = pl.BlockSpec((1, rows, part), lambda i, q: (layer, q[0], t * steps + i))
        state = pl.BlockSpec((1, rows, part), lambda i, q: (layer, 0, t * steps + i))
        kept = pl.BlockSpec((1, pairs, rows, part), lambda i, q: (q[0] // 2, 0, 0, i))
        flat = pl.BlockSpec((pairs, rows, part), lambda i, q: (0, 0, i))
    else:
        rows, width, steps = TILE, D, 4
        part = rows // steps
        mine = pl.BlockSpec((1, part, width), lambda i, q: (layer, q[0] * steps + i, 0))
        state = pl.BlockSpec((1, part, width), lambda i, q: (layer, i, 0))
        kept = pl.BlockSpec((1, pairs, part, width), lambda i, q: (q[0] // 2, 0, i, 0))
        flat = pl.BlockSpec((pairs, part, width), lambda i, q: (0, i, 0))
    specs = [mine, state, state] * pairs
    shapes = [sds(a.shape, a.dtype) for a in arrays]
    anys = [pl.BlockSpec(memory_space=pl.ANY)] * len(chain)
    alias = {4 + 3 * pairs + i: i for i in range(len(chain))}
    out = pl.pallas_call(
        functools.partial(update_body, pairs),
        grid_spec=pltpu.PrefetchScalarGridSpec(
            num_scalar_prefetch=1, grid=(steps,), in_specs=[kept, kept, flat, *specs, *anys], out_specs=[*specs, flat]
        ),
        out_shape=[*shapes, sds((pairs, rows, width), BF)],
        input_output_aliases=alias,
        compiler_params=params(),
        cost_estimate=pl.CostEstimate(flops=10**8, bytes_accessed=8 * 10**6, transcendentals=0),
        name="update",
    )(q, keep, near, got, *arrays, *chain)
    return list(out[:-1]), out[-1]


def place_body(pairs, q_ref, near_ref, far_ref, diagonal_ref, *refs):
    outs = refs[-pairs:]
    step = pl.program_id(0)
    for k, piece in enumerate((near_ref, far_ref, diagonal_ref)):

        @pl.when(step == k)
        def _():
            for i in range(pairs):
                outs[i][0] = piece[i]


def place(layer, t, q, near, far, diagonal, chain):
    pairs = len(chain)
    rows, width = near.shape[1:]
    whole = pl.BlockSpec((pairs, rows, width), lambda i, q: (0, 0, 0))
    spec = pl.BlockSpec((1, rows, width), lambda i, q: (layer, q[0] ^ (i + 1), t))
    return list(
        pl.pallas_call(
            functools.partial(place_body, pairs),
            grid_spec=pltpu.PrefetchScalarGridSpec(
                num_scalar_prefetch=1,
                grid=(3,),
                in_specs=[whole] * 3 + [pl.BlockSpec(memory_space=pl.ANY)] * pairs,
                out_specs=[spec] * pairs,
            ),
            out_shape=[jax.ShapeDtypeStruct(a.shape, a.dtype) for a in chain],
            input_output_aliases={4 + i: i for i in range(pairs)},
            compiler_params=params(),
            cost_estimate=pl.CostEstimate(flops=10**7, bytes_accessed=7 * 10**6, transcendentals=0),
            name="place",
        )(q, near, far, diagonal, *chain)
    )


def after(x, *deps):
    return lax.optimization_barrier((x, *deps))[0]


def sum_body(q_ref, keep_ref, got_ref, o_ref):
    o_ref[...] = (keep_ref[0] + got_ref[0].astype(F32)).astype(BF)


def sum_far(q, keep, got):
    shape = keep.shape[1:]
    part = (*shape[:-1], shape[-1] // 3)
    spec = pl.BlockSpec((1, *part), lambda i, q: (1 - q[0] // 2, 0, 0, i))
    return pl.pallas_call(
        sum_body,
        grid_spec=pltpu.PrefetchScalarGridSpec(
            num_scalar_prefetch=1, grid=(3,), in_specs=[spec, spec], out_specs=pl.BlockSpec(part, lambda i, q: (0, 0, i))
        ),
        out_shape=jax.ShapeDtypeStruct(shape, BF),
        compiler_params=params(),
        cost_estimate=pl.CostEstimate(flops=10**7, bytes_accessed=4 * 10**6, transcendentals=0),
        name="sum_far",
    )(q, keep, got)


def solution(mesh):
    def body(x, dy, wg, wu, wd, mg, mu, md, vg, vu, vd):
        x, dy = x[0], dy[0]
        q = lax.axis_index("dp").reshape(1)
        gate_up, downs = (wg, mg, vg, wu, mu, vu), (wd, md, vd)
        last = [None]
        chains = {2: [], 1: []}

        def run(f, first, *args):
            if last[0] is not None:
                first = after(first, *last[0])
            out = f(first, *args)
            last[0] = [jax.tree.leaves(out)[-1]]
            return out

        def send(x, pairs):
            return lax.ppermute(x, "dp", pairs)

        class Chunk:
            def __init__(self, layer, t, keep, out):
                self.layer, self.t, self.keep = layer, t, keep
                self.pairs = keep.shape[1]
                self.got = send(out, SIBLING)

            def cross(self):
                far = run(lambda keep: sum_far(q, keep, self.got), self.keep)
                self.far = send(far, CROSS)

            def update(self):
                arrays = gate_up if self.pairs == 2 else downs
                chain = chains[self.pairs]
                chain, w = run(lambda keep: update(self.layer, self.t, q, keep, self.got, self.far, arrays, chain), self.keep)
                chains[self.pairs] = chain
                self.wfar = send(w, CROSS)
                self.wnear = send(w, SIBLING)

            def forward(self):
                self.wdiag = send(self.wfar, SIBLING)

            def place(self):
                chain = chains[self.pairs]
                at = list(range(0, 3 * self.pairs, 3))
                placed = run(lambda near: place(self.layer, self.t, q, near, self.wfar, self.wdiag, [chain[i] for i in at]), self.wnear)
                for i, p in zip(at, placed):
                    chain[i] = p

        g0, u0, a0, h1, a1 = run(lambda x: fwd(x, wg, wu, wd), x)
        c, outs = [], []

        def back1(t):
            act, dg, du, keep, out = run(lambda a: back(1, t, q, dy, a, wg, wu, wd), a1)
            outs.append((act, dg, du))
            c.append(Chunk(1, t, keep, out))

        def down_of(layer, acts, d):
            keep, out = run(lambda d: down(q, acts, d), d)
            c.append(Chunk(layer, 0, keep[:, None], out[:, None]))

        back1(0)
        c[0].cross()
        back1(1)
        c[1].cross()
        c[0].update()
        back1(2)
        c[2].cross()
        c[1].update()
        back1(3)
        c[0].forward()
        c[3].cross()
        c[2].update()
        down_of(1, [o[0] for o in outs], dy)
        c[1].forward()
        c[0].place()
        d = run(lambda h: input_grad(dy, h, [o[1] for o in outs], [o[2] for o in outs], wg, wu), h1)
        c[4].cross()
        c[3].update()
        c[2].forward()
        c[1].place()
        acts = []
        for t in range(4):
            act, keep, out = run(lambda d: back(0, t, q, d, a0, g0, u0, wd), d)
            acts.append(act)
            c.append(Chunk(0, t, keep, out))
            if t:
                c[4 + t].cross()
            if t == 0:
                c[2].place()
                c[3].forward()
            if t == 1:
                c[4].update()
            if t == 2:
                c[3].place()
            if t == 3:
                c[5].update()
        down_of(0, acts, d)
        c[8].cross()
        c[4].forward()
        c[6].update()
        c[9].cross()
        c[5].forward()
        c[4].place()
        c[7].update()
        c[6].forward()
        c[5].place()
        c[8].update()
        c[7].forward()
        c[6].place()
        c[9].update()
        c[8].forward()
        c[7].place()
        c[8].place()
        c[9].forward()
        c[9].place()
        g, o = chains[2], chains[1]
        return g[0], g[3], o[0], g[1], g[4], o[1], g[2], g[5], o[2]

    batch, whole, rows = P(("rep", "dp")), P(), P(None, "dp")

    step = jax.shard_map(
        body,
        mesh=mesh,
        in_specs=(batch, batch, *(whole,) * 3, *(rows,) * 6),
        out_specs=(*(P("rep"),) * 3, *(P("rep", "dp"),) * 6),
        check_vma=False,
    )
    shape = lambda dtype, *s: jax.ShapeDtypeStruct(s, dtype)
    tokens = shape(BF, mesh.size, T, D)
    weights = [shape(BF, 2, D, FF)] * 2 + [shape(BF, 2, FF, D)]
    states = [shape(F32, *w.shape) for w in weights]
    jax.eval_shape(step, tokens, tokens, *weights, *states, *states)
    return step
```
